512 devices in a mesh: rows: 128 (over z, y, core), feat: 4 (over x).
Axes of the slice: x: 4, y: 8, z: 8, core: 2. Of those that a mesh axis runs over, the one named last changes fastest.
Arguments:
- codes: int32 [262144, 512], P('rows', 'feat'), may hold values from 0 to 31
- node_ids: int32 [262144], P('rows'), may hold values from 0 to 127
- bag: int32 [262144], P('rows'), may hold values from 0 to 3
- response: bfloat16 [262144], P('rows'), may hold values from -6 to 6
- owner_slot: int32 [128], replicated, may hold values from 0 to 127, each once
- chosen_feature: int32 [128], replicated, may hold values from 0 to 511
- chosen_bin: int32 [128], replicated, may hold values from 0 to 30
Outputs:
- gains: float32 [128, 16384], P('rows', 'feat')
- best_gain: float32 [128], P('rows')
- child_ids: int32 [262144], P('rows')
The draws below stay inside these ranges and needn't reach their ends.
All inputs are finite; a program needn't handle non-finite values.
Results may differ from the reference program's by a relative error of at most 0.0003.
Values sent between devices are 32-bit elements; how exact they have to be, the bound alone decides.
A program may use at most 64 MiB of HBM per device.

```python
import math
import jax
import jax.numpy as jnp
import numpy as np
from jax import lax

FEAT = 512
BINS = 32
NODES = 128
ROWS = 262144


def with_ends(array, stream_key, low, largest):
    place = [jax.random.randint(jax.random.fold_in(stream_key, axis), (), 0, length) for axis, length in enumerate(array.shape)]
    main_axis = array.shape.index(max(array.shape))
    beside = place[:main_axis] + [(place[main_axis] + 1) % array.shape[main_axis]] + place[main_axis + 1:]
    return array.at[tuple(place)].set(low).at[tuple(beside)].set(largest)


def level_of(key, dims, shards, smallest, top_value):
    gain, own = 1.0, jax.random.fold_in(key, 6)
    for axis_at, shards_of in shards:
        heights = jnp.exp(jax.random.uniform(jax.random.fold_in(own, axis_at), (shards_of,), jnp.float32, smallest / len(shards), top_value / len(shards)))
        gain = gain * jnp.repeat(heights, dims[axis_at] // shards_of).reshape([-1 if axis == axis_at else 1 for axis in range(len(dims))])
    return gain


def cumulative_ranks(amount, slope):
    loads = [(1 << 20) // math.isqrt(standing ** slope) + 1 for standing in range(1, amount + 1)]
    scale = 1 + sum(loads) // (1 << 30)
    return np.cumsum(np.array([max(1, weight // scale) for weight in loads]))


def skewed_ids(rng, dims, count, lean):
    grid = cumulative_ranks(count, lean)
    ticket = jax.random.randint(jax.random.fold_in(rng, 1), dims, 0, int(grid[count - 1]))
    standing = jnp.searchsorted(jnp.asarray(grid, jnp.int32), ticket, side="right")
    return jax.random.permutation(jax.random.fold_in(rng, 2), count)[standing].astype(jnp.int32)


def gaussian(stream_key, extent, scale, most, split=(), kind=jnp.bfloat16):
    values = scale * jax.random.normal(stream_key, extent, jnp.float32)
    if split:
        values = values * level_of(stream_key, extent, split, -0.22, 0.18)
    return jnp.clip(values, -most, most).astype(kind)


def setup_inputs(seed: int = 0) -> dict:
    streams_of = jax.random.split(jax.random.key(seed), 8)
    return {
        "codes": with_ends(jax.random.randint(streams_of[0], (ROWS, FEAT), 0, BINS), jax.random.fold_in(streams_of[0], 1), 0, BINS - 1).astype(jnp.int32),
        "node_ids": with_ends(skewed_ids(streams_of[1], (ROWS,), NODES, 2), jax.random.fold_in(streams_of[1], 3), 0, NODES - 1).astype(jnp.int32),
        "bag": with_ends(jax.random.randint(streams_of[2], (ROWS,), 0, 4), jax.random.fold_in(streams_of[2], 1), 0, 3).astype(jnp.int32),
        "response": gaussian(streams_of[3], (ROWS,), 1.0, 6.0, ((0, 128),)),
        "owner_slot": jax.random.permutation(streams_of[4], NODES).astype(jnp.int32),
        "chosen_feature": with_ends(jax.random.randint(streams_of[5], (NODES,), 0, FEAT), jax.random.fold_in(streams_of[5], 1), 0, FEAT - 1).astype(jnp.int32),
        "chosen_bin": with_ends(jax.random.randint(streams_of[6], (NODES,), 0, BINS - 1), jax.random.fold_in(streams_of[6], 1), 0, (BINS - 1) - 1).astype(jnp.int32),
    }


LAMBDA = 1.0


def reference(codes, node_ids, bag, response, owner_slot, chosen_feature, chosen_bin):
    weight = bag.astype(jnp.float32)
    grad = weight * response.astype(jnp.float32)
    slot = owner_slot[node_ids]
    block = 64
    count = codes.shape[0]

    def per_block(index):
        piece = lax.dynamic_slice_in_dim(codes, (index * block).astype(jnp.int32), block, 1)
        seg = slot[:, None] * (block * BINS) + jnp.arange(block, dtype=jnp.int32)[None, :] * BINS + piece
        seg = seg.reshape(-1)
        hw = jax.ops.segment_sum(jnp.broadcast_to(weight[:, None], (count, block)).reshape(-1), seg, NODES * block * BINS)
        hg = jax.ops.segment_sum(jnp.broadcast_to(grad[:, None], (count, block)).reshape(-1), seg, NODES * block * BINS)
        return jnp.stack([hw.reshape(NODES, block * BINS), hg.reshape(NODES, block * BINS)])

    stacked = lax.map(per_block, jnp.arange(FEAT // block, dtype=jnp.int32))
    stacked = stacked.transpose(1, 2, 0, 3).reshape(2, NODES, FEAT, BINS)
    hist_w, hist_g = stacked[0], stacked[1]
    left_w = jnp.cumsum(hist_w, axis=2)
    left_g = jnp.cumsum(hist_g, axis=2)
    total_w = jnp.sum(hist_w, axis=2, keepdims=True)
    total_g = jnp.sum(hist_g, axis=2, keepdims=True)
    right_w = total_w - left_w
    right_g = total_g - left_g
    gains = left_g * left_g / (left_w + LAMBDA) + right_g * right_g / (right_w + LAMBDA) - total_g * total_g / (total_w + LAMBDA)
    gains = gains.reshape(NODES, FEAT * BINS)
    best_gain = jnp.max(gains, axis=1)
    feat_row = chosen_feature[node_ids]
    code = jnp.take_along_axis(codes, feat_row[:, None], axis=1)[:, 0]
    right = (code > chosen_bin[node_ids]).astype(jnp.int32)
    child_ids = 2 * node_ids + right
    return gains, best_gain, child_ids
```

```python
import functools

import jax
import jax.numpy as jnp
from jax import lax
from jax.experimental import pallas as pl
from jax.experimental.pallas import tpu as pltpu
from jax.sharding import Mesh
from jax.sharding import PartitionSpec as P

BINS = 32
LAMBDA = 1.0
RING = 8
FEATS = 4
NODES = 128
ROWS = 2048
TILES = ROWS // 128
CHUNK = 8
CHUNKS = 8
WIDE = CHUNK * BINS
LONG = RING // 2
SHORT = RING // 2 - 1
LAG = 4
LAG2 = 4
MESH = pl.DeviceIdType.MESH
NT = (((1,), (1,)), ((), ()))


def iota(shape, dim):
    return lax.broadcasted_iota(jnp.int32, shape, dim)


def kernel(
    codes_ref, node_ref, bag_ref, resp_ref, slot_ref, feat_ref, bin_ref,
    gains_ref, best_ref, child_ref,
    turned, meta, flags, pick, spread_a, spread_b, hist, ring, part, arrived, gain_rows, gain_in,
    top, tops, node_of, bin_of,
    swap_send, swap_recv, flag_send, flag_recv, ring_send, ring_recv, far_send, far_recv,
    top_send, top_recv, gain_send, gain_recv,
):
    z, y, core, x = (lax.axis_index(name) for name in ("z", "y", "c", "x"))
    near = (1 - core) * z + core * y
    far = core * z + (1 - core) * y

    def along_near(place):
        return {"z": (1 - core) * place + core * z, "y": core * place + (1 - core) * y}

    def along_far(place):
        return {"z": core * place + (1 - core) * z, "y": (1 - core) * place + core * y}

    def wrap(place):
        return lax.rem(place + 2 * RING, RING)

    other = {"c": 1 - core}
    beside = [
        {"x": lax.rem(x + dx, FEATS), "c": lax.rem(core + dc, 2)}
        for dx in range(FEATS)
        for dc in range(2)
        if dx or dc
    ]

    barrier = pltpu.get_barrier_semaphore()
    greeted = [along_near(wrap(near + 1)), along_near(wrap(near - 1))]
    greeted += [along_far(wrap(far + step)) for step in range(1, RING)]
    greeted += beside
    for peer in greeted:
        pl.semaphore_signal(barrier, inc=1, device_id=peer, device_id_type=MESH)

    def remote(src, dst, send, recv, peer):
        return pltpu.make_async_remote_copy(
            src_ref=src, dst_ref=dst, send_sem=send, recv_sem=recv, device_id=peer, device_id_type=MESH
        )

    meta[0, 0] = node_ref[...].astype(jnp.float32)
    meta[0, 1] = bag_ref[...].astype(jnp.float32)
    meta[0, 2] = resp_ref[...].astype(jnp.float32)

    lane = iota((NODES, 128), 1)
    line = iota((NODES, 128), 0)
    feat_col = jnp.sum(jnp.where(lane == line, feat_ref[...], 0), axis=1, keepdims=True)
    bin_col = jnp.sum(jnp.where(lane == line, bin_ref[...], 0), axis=1, keepdims=True)
    same = jnp.where(lane == line, 1.0, 0.0).astype(jnp.bfloat16)
    split = jnp.where(lane == feat_col - x * 128, 1.0, 0.0).astype(jnp.bfloat16)
    bin_of[...] = jnp.broadcast_to(bin_col.astype(jnp.float32), (NODES, 128))
    both = jnp.concatenate([same, split], axis=0)
    line_f = line.astype(jnp.float32)
    for turn in range(ROWS // 256):
        rows = pl.ds(turn * 256, 256)
        part_codes = codes_ref[rows, :].astype(jnp.float32).astype(jnp.bfloat16)
        out = lax.dot_general(both, part_codes, NT, preferred_element_type=jnp.float32)
        for half in range(2):
            for chunk in range(CHUNKS):
                at = half * 64 + chunk * CHUNK
                turned[half, chunk, :, rows] = out[at : at + CHUNK]
        for sub in range(2):
            tile = turn * 2 + sub
            code = out[NODES:, sub * 128 : (sub + 1) * 128]
            mine = (line_f == meta[0, 0, tile : tile + 1, :]) & (code > bin_of[...])
            flags[x, tile : tile + 1, :] = jnp.sum(jnp.where(mine, 1.0, 0.0), axis=0, keepdims=True)

    pl.semaphore_wait(barrier, len(greeted))

    swap = [
        remote(turned.at[1 - core], turned.at[2], swap_send.at[0], swap_recv.at[0], other),
        remote(meta.at[0], meta.at[1], swap_send.at[1], swap_recv.at[1], other),
    ]
    for copy in swap:
        copy.start()
    flag_copies = [
        remote(
            flags.at[x], flags.at[x], flag_send.at[dx - 1], flag_recv.at[dx - 1], {"x": lax.rem(x + dx, FEATS)}
        )
        for dx in range(1, FEATS)
    ]
    for copy in flag_copies:
        copy.start()

    lane = iota((2 * NODES, 128), 1)
    line = iota((2 * NODES, 128), 0)
    near_size = (1 - core) * 16 + core * 2
    far_size = (1 - core) * 2 + core * 16
    wanted = (line // 32) * near_size + (lax.rem(line, 32) // 4) * far_size + lax.rem(line, 2)
    node_col = jnp.sum(jnp.where(slot_ref[...] == wanted, lane, 0), axis=1, keepdims=True)
    node_of[...] = jnp.broadcast_to(node_col.astype(jnp.float32), (2 * NODES, 128))
    weigh = lax.rem(iota((8, 128), 0), 4) < 2

    def fill_pick(source):
        for tile in range(TILES):
            node = meta[source, 0, tile : tile + 1, :]
            value = jnp.where(weigh, 1.0, meta[source, 2, tile : tile + 1, :])
            value = jnp.concatenate([value] * (2 * NODES // 8), axis=0)
            block = jnp.where(node_of[...] == node, value, 0.0).astype(jnp.bfloat16)
            pick[:, source * ROWS + tile * 128 : source * ROWS + (tile + 1) * 128] = block

    bins = iota((BINS, 128), 0).astype(jnp.bfloat16)

    def fill_spread(spread, chunk):
        for source in range(2):
            where = core if source == 0 else 2
            for tile in range(TILES):
                at = slice(tile * 128, (tile + 1) * 128)
                weight = jnp.broadcast_to(meta[source, 1, tile : tile + 1, :], (BINS, 128)).astype(jnp.bfloat16)
                for feature in range(CHUNK):
                    code = jnp.broadcast_to(turned[where, chunk, feature : feature + 1, at], (BINS, 128))
                    code = code.astype(jnp.bfloat16)
                    spread[
                        feature * BINS : (feature + 1) * BINS, source * ROWS + tile * 128 : source * ROWS + (tile + 1) * 128
                    ] = jnp.where(code <= bins, weight, jnp.zeros_like(weight))

    fill_pick(0)
    for copy in swap:
        copy.wait_recv()
    fill_pick(1)
    fill_spread(spread_a, 0)

    def ring_copy(chunk, step, is_long):
        way = 1 - 2 * lax.rem(chunk, 2)
        if not is_long:
            way = -way
        at = step - 1 + (0 if is_long else LONG)
        length = LONG if is_long else SHORT
        owner = wrap(near + way * (length + 1 - step))
        if step == 1:
            src = hist.at[chunk, pl.ds(pl.multiple_of(owner * 32, 32), 32), :]
        else:
            src = ring.at[chunk, at - 1]
        peer = along_near(wrap(near + way))
        return remote(src, ring.at[chunk, at], ring_send.at[chunk, at], ring_recv.at[chunk, at], peer), owner

    def ring_step(chunk, step, is_long):
        copy, owner = ring_copy(chunk, step, is_long)
        if step > 1:
            ring_copy(chunk, step - 1, is_long)[0].wait_recv()
            at = step - 2 + (0 if is_long else LONG)
            ring[chunk, at] = ring[chunk, at] + hist[chunk, pl.ds(pl.multiple_of(owner * 32, 32), 32), :]
        copy.start()

    def far_copy(chunk, step):
        place = wrap(far + step)
        return remote(
            part.at[chunk, place], arrived.at[chunk, far], far_send.at[chunk, step - 1], far_recv.at[chunk, step - 1],
            along_far(place),
        )

    def ring_end(chunk):
        ring_copy(chunk, LONG, True)[0].wait_recv()
        ring_copy(chunk, SHORT, False)[0].wait_recv()
        mine = hist[chunk, pl.ds(pl.multiple_of(near * 32, 32), 32), :]
        mine = mine + ring[chunk, LONG - 1] + ring[chunk, LONG + SHORT - 1]
        for place in range(RING):
            part[chunk, place] = mine[place * 4 : place * 4 + 4]
        arrived[chunk, far] = part[chunk, far]
        for step in range(1, RING):
            far_copy(chunk, step).start()

    last = lax.rem(iota((2, WIDE), 1), BINS) == BINS - 1

    def spread_last(row):
        row = jnp.where(last, row, 0.0)
        for shift in (1, 2, 4, 8, 16):
            row = row + pltpu.roll(row, WIDE - shift, 1)
        return row

    def chunk_gains(chunk):
        for step in range(1, RING):
            far_copy(chunk, step).wait_recv()
        mine = arrived[chunk, 0]
        for place in range(1, RING):
            mine = mine + arrived[chunk, place]
        left_w, left_g = mine[0:2], mine[2:4]
        total_w, total_g = spread_last(left_w), spread_last(left_g)
        right_w, right_g = total_w - left_w, total_g - left_g
        gains = (
            left_g * left_g / (left_w + LAMBDA)
            + right_g * right_g / (right_w + LAMBDA)
            - total_g * total_g / (total_w + LAMBDA)
        )
        at = pl.ds(pl.multiple_of(chunk * WIDE, WIDE), WIDE)
        gain_rows[0, :, at] = gains[0:1]
        gain_rows[1, :, at] = gains[1:2]

    def compute(chunk, spread, following):
        @pl.when(chunk < CHUNKS)
        def _():
            hist[chunk] = lax.dot_general(pick[...], spread[...], NT, preferred_element_type=jnp.float32)
            fill_spread(following, lax.rem(chunk + 1, CHUNKS))

    def moves(slot):
        def stage(lag, work):
            chunk = slot - lag

            @pl.when((chunk >= 0) & (chunk < CHUNKS))
            def _():
                work(chunk)

        for step in range(1, LONG + 1):
            def work(chunk, step=step):
                ring_step(chunk, step, True)
                if step <= SHORT:
                    ring_step(chunk, step, False)
            stage(LAG * (step - 1), work)
        stage(LAG * LONG, ring_end)
        stage(LAG * LONG + LAG2, chunk_gains)

    slots = CHUNKS + LAG * LONG + LAG2

    def pair(index, carry):
        compute(2 * index, spread_a, spread_b)
        moves(2 * index)
        compute(2 * index + 1, spread_b, spread_a)
        moves(2 * index + 1)
        return carry

    lax.fori_loop(0, (slots + 1) // 2, pair, 0)

    for node in range(2):
        largest = jnp.max(gain_rows[node], axis=1, keepdims=True)
        top[node] = jnp.broadcast_to(largest, (1, 128))
    tops[x * 2 + core] = top[core]
    top_copies = [
        remote(top.at[peer["c"]], tops.at[x * 2 + core], top_send.at[index], top_recv.at[index], peer)
        for index, peer in enumerate(beside)
    ]
    gain_copy = remote(gain_rows.at[1 - core], gain_in, gain_send, gain_recv, other)
    for copy in top_copies:
        copy.start()
    gain_copy.start()

    for copy in flag_copies:
        copy.wait_recv()
    right = flags[0] + flags[1] + flags[2] + flags[3]
    child_ref[...] = 2 * node_ref[...] + jnp.where(right > 0.5, 1, 0)

    for copy in swap + flag_copies:
        copy.wait_send()

    def drain(chunk, carry):
        for step in range(1, LONG + 1):
            ring_copy(chunk, step, True)[0].wait_send()
        for step in range(1, SHORT + 1):
            ring_copy(chunk, step, False)[0].wait_send()
        for step in range(1, RING):
            far_copy(chunk, step).wait_send()
        return carry

    lax.fori_loop(0, CHUNKS, drain, 0)

    gain_copy.wait_recv()
    own, got = gain_rows[core], gain_in[...]
    half = CHUNKS * WIDE
    gains_ref[:, :half] = jnp.where(core == 0, own, got)
    gains_ref[:, half:] = jnp.where(core == 0, got, own)
    for copy in top_copies:
        copy.wait_recv()
    best = tops[0]
    for place in range(1, 2 * FEATS):
        best = jnp.maximum(best, tops[place])
    best_ref[...] = best[:, :1]
    for copy in top_copies + [gain_copy]:
        copy.wait_send()


def per_device(codes, node_ids, bag, response, owner_slot, chosen_feature, chosen_bin):
    vmem = pl.BlockSpec(memory_space=pltpu.VMEM)
    f32 = jnp.float32
    dma = pltpu.SemaphoreType.DMA
    gains, best, child = pl.pallas_call(
        kernel,
        out_shape=(
            jax.ShapeDtypeStruct((1, 128 * BINS), f32),
            jax.ShapeDtypeStruct((1, 1), f32),
            jax.ShapeDtypeStruct((TILES, 128), jnp.int32),
        ),
        in_specs=[vmem] * 7,
        out_specs=(vmem, vmem, vmem),
        scratch_shapes=[
            pltpu.VMEM((3, CHUNKS, CHUNK, ROWS), f32),
            pltpu.VMEM((2, 3, TILES, 128), f32),
            pltpu.VMEM((FEATS, TILES, 128), f32),
            pltpu.VMEM((2 * NODES, 2 * ROWS), jnp.bfloat16),
            pltpu.VMEM((WIDE, 2 * ROWS), jnp.bfloat16),
            pltpu.VMEM((WIDE, 2 * ROWS), jnp.bfloat16),
            pltpu.VMEM((CHUNKS, 2 * NODES, WIDE), f32),
            pltpu.VMEM((CHUNKS, LONG + SHORT, 32, WIDE), f32),
            pltpu.VMEM((CHUNKS, RING, 4, WIDE), f32),
            pltpu.VMEM((CHUNKS, RING, 4, WIDE), f32),
            pltpu.VMEM((2, 1, CHUNKS * WIDE), f32),
            pltpu.VMEM((1, CHUNKS * WIDE), f32),
            pltpu.VMEM((2, 1, 128), f32),
            pltpu.VMEM((2 * FEATS, 1, 128), f32),
            pltpu.VMEM((2 * NODES, 128), f32),
            pltpu.VMEM((NODES, 128), f32),
            dma((2,)), dma((2,)),
            dma((FEATS - 1,)), dma((FEATS - 1,)),
            dma((CHUNKS, LONG + SHORT)), dma((CHUNKS, LONG + SHORT)),
            dma((CHUNKS, RING - 1)), dma((CHUNKS, RING - 1)),
            dma((2 * FEATS - 1,)), dma((2 * FEATS - 1,)),
            dma, dma,
        ],
        compiler_params=pltpu.CompilerParams(collective_id=0, has_side_effects=True),
        name="level_step",
    )(
        codes,
        node_ids.reshape(TILES, 128),
        bag.reshape(TILES, 128),
        response.reshape(TILES, 128),
        owner_slot.reshape(1, NODES),
        chosen_feature.reshape(1, NODES),
        chosen_bin.reshape(1, NODES),
    )
    return gains, best.reshape(1), child.reshape(ROWS)


def solution(mesh):
    split = Mesh(mesh.devices.reshape(RING, RING, 2, FEATS), ("z", "y", "c", "x"))
    rows = ("z", "y", "c")
    placed = (P(rows, "x"), P(rows), P(rows), P(rows), P(), P(), P())
    return jax.shard_map(
        per_device,
        mesh=split,
        in_specs=placed,
        out_specs=(P(rows, "x"), P(rows), P(rows)),
        check_vma=False,
    )
```
